32 devices in a mesh: groups: 2 (over y), date: 4 (over z), tile: 4 (over x, core).
Axes of the slice: x: 2, y: 2, z: 4, core: 2. Of those that a mesh axis runs over, the one named last changes fastest.
Arguments:
- acquired: float32 [2, 32, 128, 128], P(None, 'date', ('groups', 'tile')), parts along dimension 2, may hold values from -10 to 10, as said below
Outputs:
- coherence: float32 [2, 4, 32, 8, 128, 128], P(None, None, 'date', None, ('groups', 'tile')), parts along dimension 4
The draws below stay inside these ranges and needn't reach their ends.
There are 2 independent parts, one for each index of `groups`. The reference program is written for one: setup_inputs(seed, part) draws one part's arguments, and reference() takes and returns one part's arrays. A program takes and returns all parts, laid end to end along the dimension named above; each array names one. Nothing has to cross between parts.
Inputs may be any that keep to these rules, and one draw needn't show every extreme that they name: `acquired`: every pixel's magnitude, the square root of the sum of its two parts squared, lies between 0.1 and 10.
All inputs are finite; a program needn't handle non-finite values.
Results may differ from the reference program's by a relative error of at most 0.000058.
Values sent between devices are 32-bit elements; how exact they have to be, the bound alone decides.
No kernel may reach another device: no remote copies, remote signals or barrier semaphores. Data moves between devices by JAX's collectives and lax.ppermute only.
A program may use at most 64 MiB of HBM per device.

```python
import math
import jax
import jax.numpy as jnp
from jax import lax

DATE_DEV = 8
SHIFTS = 4
COLS = 128
DATES = 32
ROWS = 64


def draw_acquired(key, part):
    key_mag = jax.random.fold_in(key, 11)
    key_common = jax.random.fold_in(key, 12)
    key_ramp = jax.random.fold_in(key, 13)
    key_speckle = jax.random.fold_in(key, 14)
    lowest = 0.3
    highest = 3.0
    spread = 0.8
    magnitude = jnp.exp(jax.random.uniform(key_mag, (DATES, ROWS, COLS), jnp.float32, math.log(lowest), math.log(highest)))
    common_phase = jax.random.uniform(key_common, (1, ROWS, COLS), jnp.float32, -math.pi, math.pi)
    date_ramp = jax.random.uniform(key_ramp, (DATES, 1, 1), jnp.float32, -0.5, 0.5) * jnp.arange(COLS, dtype=jnp.float32)[None, None, :]
    speckle = spread * jax.random.normal(key_speckle, (DATES, ROWS, COLS), jnp.float32)
    phases = common_phase + date_ramp + speckle
    return jnp.stack([magnitude * jnp.cos(phases), magnitude * jnp.sin(phases)]).astype(jnp.float32)


def setup_inputs(seed: int = 0, part: int = 0) -> dict:
    key_list = jax.random.split(jax.random.key(seed), 2)
    part_keys = jax.random.split(jax.random.fold_in(key_list[1], part), 2)
    acquired = draw_acquired(jax.random.fold_in(jax.random.fold_in(key_list[1], part), 71), part)
    return {"acquired": acquired}


row_reach = 5
col_reach = 2

def box_sum(values_in):
    height = values_in.shape[-2]
    breadth = values_in.shape[-1]
    widths = [(0, 0)] * (values_in.ndim - 2) + [(row_reach, row_reach), (col_reach, col_reach)]
    padded = jnp.pad(values_in, widths)
    summed = padded[..., 0:height, :]
    for shift_at in range(1, 2 * row_reach + 1):
        summed = summed + padded[..., shift_at:shift_at + height, :]
    result = summed[..., 0:breadth]
    for shift_at in range(1, 2 * col_reach + 1):
        result = result + summed[..., shift_at:shift_at + breadth]
    return result

def reference(acquired):
    dates_all = acquired.shape[1]
    height = acquired.shape[2]
    breadth = acquired.shape[3]
    nblocks = dates_all // DATE_DEV
    power = box_sum(acquired[0] * acquired[0] + acquired[1] * acquired[1])
    blocks = []
    for offset in range(SHIFTS):
        partner = jnp.roll(acquired, -offset * DATE_DEV, axis=1)
        partner_power = jnp.roll(power, -offset * DATE_DEV, axis=0)
        anchor = acquired.reshape(2, nblocks, DATE_DEV, 1, height, breadth)
        other = partner.reshape(2, nblocks, 1, DATE_DEV, height, breadth)
        cross_re = box_sum(anchor[0] * other[0] + anchor[1] * other[1])
        cross_im = box_sum(anchor[1] * other[0] - anchor[0] * other[1])
        inverse = lax.rsqrt(power.reshape(nblocks, DATE_DEV, 1, height, breadth) * partner_power.reshape(nblocks, 1, DATE_DEV, height, breadth))
        block = jnp.stack([cross_re * inverse, cross_im * inverse])
        blocks.append(block.reshape(2, dates_all, DATE_DEV, height, breadth))
    return jnp.stack(blocks, axis=1)
```

```python
import jax
import jax.numpy as jnp
from jax import lax
from jax.experimental import pallas as pl
from jax.experimental.pallas import tpu as pltpu
from jax.sharding import PartitionSpec as P

SHIFTS = 4

row_reach = 5
col_reach = 2


def window_sums(rows, reach, count):
    total = len(rows)
    suffix, prefix = {}, {}
    for start in range(0, total, reach):
        stop = min(start + reach, total)
        prefix[start] = rows[start]
        for i in range(start + 1, stop):
            prefix[i] = prefix[i - 1] + rows[i]
        if stop - start == reach:
            suffix[stop - 1] = rows[stop - 1]
            for i in range(stop - 2, start, -1):
                suffix[i] = suffix[i + 1] + rows[i]
    out = []
    for i in range(count):
        if i % reach == 0:
            out.append(prefix[i + reach - 1])
        else:
            out.append(suffix[i] + prefix[i + reach - 1])
    return out


def column_sums(rows, band):
    value = jnp.concatenate(rows, axis=0)
    high = value.astype(jnp.bfloat16)
    low = (value - high.astype(jnp.float32)).astype(jnp.bfloat16)
    return jnp.dot(
        jnp.concatenate([high, low], axis=1), band, preferred_element_type=jnp.float32
    )


def kernel_body(
    blocks, axis, edge_ref, mid_ref, even_ref, odd_ref, out_ref, halo, inverse, band_ref
):
    dates = edge_ref.shape[3]
    breadth = edge_ref.shape[4]
    inner = mid_ref.shape[1]
    height = inner + 2 * row_reach
    reach = 2 * row_reach + 1
    here = lax.axis_index(axis)
    count = lax.axis_size(axis)
    odd_tile = lax.rem(here, 2)

    left = lax.rem(lax.broadcasted_iota(jnp.int32, (2 * breadth, breadth), 0), breadth)
    right = lax.broadcasted_iota(jnp.int32, (2 * breadth, breadth), 1)
    band_ref[...] = (jnp.abs(left - right) <= col_reach).astype(jnp.bfloat16)
    band = band_ref[...]

    even_live = jnp.where(here == count - 1, odd_tile, 1) == 1
    odd_live = jnp.where(odd_tile == 0, here > 0, here < count - 1)
    for k in range(blocks):
        even = even_ref[k]
        odd = odd_ref[k]
        halo[k, 1 - odd_tile] = jnp.where(even_live, even, jnp.zeros_like(even))
        halo[k, odd_tile] = jnp.where(odd_live, odd, jnp.zeros_like(odd))

    def row(k, r, part, date=None):
        at = slice(None) if date is None else pl.ds(date, 1)
        if r < row_reach:
            return halo[k, 0, r, part, at, :]
        if r < 2 * row_reach:
            return edge_ref[k, r - row_reach, part, at, :]
        if r < 2 * row_reach + inner:
            return mid_ref[k, r - 2 * row_reach, part, at, :]
        if r < 3 * row_reach + inner:
            return edge_ref[k, r - row_reach - inner, part, at, :]
        return halo[k, 1, r - 3 * row_reach - inner, part, at, :]

    extent = height + 2 * row_reach
    for k in range(blocks):
        squares = []
        for r in range(extent):
            re, im = row(k, r, 0), row(k, r, 1)
            squares.append(re * re + im * im)
        power = column_sums(window_sums(squares, reach, height), band)
        inverse[k] = lax.rsqrt(power).reshape(height, dates, breadth)

    for k in range(blocks):

        def one_date(d, carry, k=k):
            real, imag = [], []
            for r in range(extent):
                a_re = jnp.broadcast_to(row(0, r, 0, d), (dates, breadth))
                a_im = jnp.broadcast_to(row(0, r, 1, d), (dates, breadth))
                b_re, b_im = row(k, r, 0), row(k, r, 1)
                real.append(a_re * b_re + a_im * b_im)
                imag.append(a_im * b_re - a_re * b_im)
            for part, values in ((0, real), (1, imag)):
                sums = column_sums(window_sums(values, reach, height), band)
                for r in range(height):
                    scale = inverse[0, r, pl.ds(d, 1), :] * inverse[k, r]
                    out_ref[part, k, d, pl.ds(r, dates, stride=height), :] = (
                        sums[r * dates : (r + 1) * dates] * scale
                    )
            return carry

        lax.fori_loop(0, dates, one_date, 0)


def coherence_of(axis, edge, mid, even, odd):
    blocks, _, _, dates, breadth = edge.shape
    height = mid.shape[1] + 2 * row_reach

    def body(*refs):
        kernel_body(blocks, axis, *refs)

    pairs = blocks * dates * dates * height * breadth
    return pl.pallas_call(
        body,
        out_shape=jax.ShapeDtypeStruct(
            (2, blocks, dates, dates * height, breadth), jnp.float32
        ),
        in_specs=[pl.BlockSpec(memory_space=pltpu.VMEM)] * 4,
        out_specs=pl.BlockSpec(memory_space=pltpu.VMEM),
        scratch_shapes=[
            pltpu.VMEM((blocks, 2, row_reach, 2, dates, breadth), jnp.float32),
            pltpu.VMEM((blocks, height, dates, breadth), jnp.float32),
            pltpu.VMEM((2 * breadth, breadth), jnp.bfloat16),
        ],
        cost_estimate=pl.CostEstimate(
            flops=pairs * 40, bytes_accessed=pairs * 8, transcendentals=0
        ),
    )(edge, mid, even, odd)


def passed_along(value, axis, steps):
    count = lax.axis_size(axis)
    pairs = [(source, (source + steps) % count) for source in range(count)]
    return lax.ppermute(value, axis, pairs)


def swapped(value, axis, first):
    count = lax.axis_size(axis)
    pairs = []
    for i in range(first, count - 1, 2):
        pairs += [(i, i + 1), (i + 1, i)]
    if first and count % 2 == 0 and count > 2:
        pairs += [(0, count - 1), (count - 1, 0)]
    return lax.ppermute(value, axis, pairs)


def on_device(acquired):
    height = acquired.shape[2]
    by_row = jnp.transpose(acquired, (2, 0, 1, 3))
    edge = jnp.concatenate([by_row[:row_reach], by_row[height - row_reach :]], axis=0)
    mid = by_row[row_reach : height - row_reach]
    edges = jnp.stack([edge] + [passed_along(edge, "date", -s) for s in range(1, SHIFTS)])
    mids = jnp.stack([mid] + [passed_along(mid, "date", -s) for s in range(1, SHIFTS)])
    odd_tile = lax.rem(lax.axis_index("tile"), 2)
    tops, bottoms = edges[:, :row_reach], edges[:, row_reach:]
    even = swapped(jnp.where(odd_tile == 0, bottoms, tops), "tile", 0)
    odd = swapped(jnp.where(odd_tile == 1, bottoms, tops), "tile", 1)
    found = coherence_of("tile", edges, mids, even, odd)
    parts, shifts, dates = found.shape[:3]
    return found.reshape(parts, shifts, dates, dates, height, found.shape[-1])


def solution(mesh):
    in_specs = (P(None, "date", ("groups", "tile"), None),)
    out_specs = P(None, None, "date", None, ("groups", "tile"), None)
    return jax.shard_map(
        on_device, mesh=mesh, in_specs=in_specs, out_specs=out_specs, check_vma=False
    )
```

```python
import jax
import jax.numpy as jnp
from jax import lax
from jax.experimental import pallas as pl
from jax.experimental.pallas import tpu as pltpu
from jax.sharding import PartitionSpec as P

SHIFTS = 4

row_reach = 5
col_reach = 2


def window_sums(rows, reach, count):
    total = len(rows)
    suffix, prefix = {}, {}
    for start in range(0, total, reach):
        stop = min(start + reach, total)
        prefix[start] = rows[start]
        for i in range(start + 1, stop):
            prefix[i] = prefix[i - 1] + rows[i]
        if stop - start == reach:
            suffix[stop - 1] = rows[stop - 1]
            for i in range(stop - 2, start, -1):
                suffix[i] = suffix[i + 1] + rows[i]
    out = []
    for i in range(count):
        if i % reach == 0:
            out.append(prefix[i + reach - 1])
        else:
            out.append(suffix[i] + prefix[i + reach - 1])
    return out


def column_sums(rows, band):
    value = jnp.concatenate(rows, axis=0)
    high = value.astype(jnp.bfloat16)
    low = (value - high.astype(jnp.float32)).astype(jnp.bfloat16)
    return jnp.dot(
        jnp.concatenate([high, low], axis=1), band, preferred_element_type=jnp.float32
    )


def kernel_body(blocks, axis, groups, unroll, *refs):
    edge_refs, mid_refs = refs[:blocks], refs[blocks : 2 * blocks]
    even_ref, odd_ref, out_ref, halo, inverse, found, sems = refs[2 * blocks :]
    _, _, dates, breadth = edge_refs[0].shape
    inner = mid_refs[0].shape[0]
    height = inner + 2 * row_reach
    reach = 2 * row_reach + 1
    here = lax.axis_index(axis)
    count = lax.axis_size(axis)
    odd_tile = lax.rem(here, 2)

    left = lax.rem(lax.broadcasted_iota(jnp.int32, (2 * breadth, breadth), 0), breadth)
    right = lax.broadcasted_iota(jnp.int32, (2 * breadth, breadth), 1)
    band = (jnp.abs(left - right) <= col_reach).astype(jnp.bfloat16)

    even_live = jnp.where(here == count - 1, odd_tile, 1) == 1
    odd_live = jnp.where(odd_tile == 0, here > 0, here < count - 1)
    for k in range(blocks):
        even = even_ref[k]
        odd = odd_ref[k]
        halo[k, 1 - odd_tile] = jnp.where(even_live, even, jnp.zeros_like(even))
        halo[k, odd_tile] = jnp.where(odd_live, odd, jnp.zeros_like(odd))

    def row(k, r, part, date=None):
        at = slice(None) if date is None else pl.ds(date, 1)
        if r < row_reach:
            return halo[k, 0, r, part, at, :]
        if r < 2 * row_reach:
            return edge_refs[k][r - row_reach, part, at, :]
        if r < 2 * row_reach + inner:
            return mid_refs[k][r - 2 * row_reach, part, at, :]
        if r < 3 * row_reach + inner:
            return edge_refs[k][r - row_reach - inner, part, at, :]
        return halo[k, 1, r - 3 * row_reach - inner, part, at, :]

    extent = height + 2 * row_reach
    for k in range(blocks):
        squares = []
        for r in range(extent):
            re, im = row(k, r, 0), row(k, r, 1)
            squares.append(re * re + im * im)
        power = column_sums(window_sums(squares, reach, height), band)
        inverse[k] = lax.rsqrt(power).reshape(height, dates, breadth)

    copies = []
    step = dates // groups
    for k in range(blocks):

        def one_date(d, carry, k=k):
            real, imag = [], []
            for r in range(extent):
                a_re = jnp.broadcast_to(row(0, r, 0, d), (dates, breadth))
                a_im = jnp.broadcast_to(row(0, r, 1, d), (dates, breadth))
                b_re, b_im = row(k, r, 0), row(k, r, 1)
                real.append(a_re * b_re + a_im * b_im)
                imag.append(a_im * b_re - a_re * b_im)
            for part, values in ((0, real), (1, imag)):
                sums = column_sums(window_sums(values, reach, height), band)
                for r in range(height):
                    scale = inverse[0, r, pl.ds(d, 1), :] * inverse[k, r]
                    found[part, k, d, pl.ds(r, dates, stride=height), :] = (
                        sums[r * dates : (r + 1) * dates] * scale
                    )
            return carry

        for g in range(groups):
            lax.fori_loop(g * step, (g + 1) * step, one_date, 0, unroll=min(unroll, step))
            for part in range(2):
                span = pl.ds(g * step, step)
                copy = pltpu.make_async_copy(
                    found.at[part, k, span], out_ref.at[part, k, span], sems.at[k, g, part]
                )
                copy.start()
                copies.append(copy)
    for copy in copies:
        copy.wait()


def coherence_of(axis, edges, mids, even, odd, groups=2, unroll=4):
    blocks = len(edges)
    _, _, dates, breadth = edges[0].shape
    height = mids[0].shape[0] + 2 * row_reach

    def body(*refs):
        kernel_body(blocks, axis, groups, unroll, *refs)

    pairs = blocks * dates * dates * height * breadth
    result = (2, blocks, dates, dates * height, breadth)
    return pl.pallas_call(
        body,
        out_shape=jax.ShapeDtypeStruct(result, jnp.float32),
        in_specs=[pl.BlockSpec(memory_space=pltpu.VMEM)] * (2 * blocks + 2),
        out_specs=pl.BlockSpec(memory_space=pl.ANY),
        scratch_shapes=[
            pltpu.VMEM((blocks, 2, row_reach, 2, dates, breadth), jnp.float32),
            pltpu.VMEM((blocks, height, dates, breadth), jnp.float32),
            pltpu.VMEM(result, jnp.float32),
            pltpu.SemaphoreType.DMA((blocks, groups, 2)),
        ],
        compiler_params=pltpu.CompilerParams(vmem_limit_bytes=16 * 1024 * 1024),
        cost_estimate=pl.CostEstimate(
            flops=pairs * 40, bytes_accessed=pairs * 8, transcendentals=0
        ),
    )(*edges, *mids, even, odd)


def passed_along(value, axis, steps):
    count = lax.axis_size(axis)
    pairs = [(source, (source + steps) % count) for source in range(count)]
    return lax.ppermute(value, axis, pairs)


def swapped(value, axis, first):
    count = lax.axis_size(axis)
    pairs = []
    for i in range(first, count - 1, 2):
        pairs += [(i, i + 1), (i + 1, i)]
    if first and count % 2 == 0 and count > 2:
        pairs += [(0, count - 1), (count - 1, 0)]
    return lax.ppermute(value, axis, pairs)


def on_device(acquired):
    height = acquired.shape[2]
    by_row = jnp.transpose(acquired, (2, 0, 1, 3))
    edge = jnp.concatenate([by_row[:row_reach], by_row[height - row_reach :]], axis=0)
    mid = by_row[row_reach : height - row_reach]
    edges = [edge] + [passed_along(edge, "date", -s) for s in range(1, SHIFTS)]
    mids = [mid] + [passed_along(mid, "date", -s) for s in range(1, SHIFTS)]
    odd_tile = lax.rem(lax.axis_index("tile"), 2)
    tops = jnp.stack([e[:row_reach] for e in edges])
    bottoms = jnp.stack([e[row_reach:] for e in edges])
    even = swapped(jnp.where(odd_tile == 0, bottoms, tops), "tile", 0)
    odd = swapped(jnp.where(odd_tile == 1, bottoms, tops), "tile", 1)
    found = coherence_of("tile", edges, mids, even, odd)
    parts, shifts, dates = found.shape[:3]
    return found.reshape(parts, shifts, dates, dates, height, found.shape[-1])


def solution(mesh):
    in_specs = (P(None, "date", ("groups", "tile"), None),)
    out_specs = P(None, None, "date", None, ("groups", "tile"), None)
    return jax.shard_map(
        on_device, mesh=mesh, in_specs=in_specs, out_specs=out_specs, check_vma=False
    )
```

```python
import jax
import jax.numpy as jnp
from jax import lax
from jax.experimental import pallas as pl
from jax.experimental.pallas import tpu as pltpu
from jax.sharding import PartitionSpec as P


SHIFTS = 4


row_reach = 5
col_reach = 2


def window_sums(rows, reach, count):
    total = len(rows)
    suffix, prefix = {}, {}
    for start in range(0, total, reach):
        stop = min(start + reach, total)
        prefix[start] = rows[start]
        for i in range(start + 1, stop):
            prefix[i] = prefix[i - 1] + rows[i]
        if stop - start == reach:
            suffix[stop - 1] = rows[stop - 1]
            for i in range(stop - 2, start, -1):
                suffix[i] = suffix[i + 1] + rows[i]
    out = []
    for i in range(count):
        if i % reach == 0:
            out.append(prefix[i + reach - 1])
        else:
            out.append(suffix[i] + prefix[i + reach - 1])
    return out


def column_sums(rows, band):
    value = jnp.concatenate(rows, axis=0)
    high = value.astype(jnp.bfloat16)
    low = (value - high.astype(jnp.float32)).astype(jnp.bfloat16)
    return jnp.dot(
        jnp.concatenate([high, low], axis=1), band, preferred_element_type=jnp.float32
    )


def kernel_body(blocks, axis, groups, unroll, *refs):
    outer_refs, rest_refs = refs[:blocks], refs[blocks : 2 * blocks]
    even_ref, odd_ref, out_ref, field, inverse, found, sems = refs[2 * blocks :]
    _, _, dates, breadth = outer_refs[0].shape
    inner = rest_refs[0].shape[0]
    height = inner + row_reach
    extent = height + 2 * row_reach
    reach = 2 * row_reach + 1
    here = lax.axis_index(axis)
    count = lax.axis_size(axis)
    odd_tile = lax.rem(here, 2)

    left = lax.rem(lax.broadcasted_iota(jnp.int32, (2 * breadth, breadth), 0), breadth)
    right = lax.broadcasted_iota(jnp.int32, (2 * breadth, breadth), 1)
    band = (jnp.abs(left - right) <= col_reach).astype(jnp.bfloat16)

    even_live = jnp.where(here == count - 1, odd_tile, 1) == 1
    odd_live = jnp.where(odd_tile == 0, here > 0, here < count - 1)
    odd_at = odd_tile * (height + row_reach)
    even_at = (1 - odd_tile) * (height + row_reach)
    outer_at = row_reach + odd_tile * inner
    rest_at = (2 - odd_tile) * row_reach
    for k in range(blocks):
        even = even_ref[k]
        odd = odd_ref[k]
        field[k, pl.ds(even_at, row_reach)] = jnp.where(even_live, even, jnp.zeros_like(even))
        field[k, pl.ds(odd_at, row_reach)] = jnp.where(odd_live, odd, jnp.zeros_like(odd))
        field[k, pl.ds(outer_at, row_reach)] = outer_refs[k][...]
        field[k, pl.ds(rest_at, inner)] = rest_refs[k][...]

    def row(k, r, part, date=None):
        at = slice(None) if date is None else pl.ds(date, 1)
        return field[k, r, part, at, :]

    for k in range(blocks):
        squares = []
        for r in range(extent):
            re, im = row(k, r, 0), row(k, r, 1)
            squares.append(re * re + im * im)
        power = column_sums(window_sums(squares, reach, height), band)
        inverse[k] = lax.rsqrt(power).reshape(height, dates, breadth)

    copies = []
    step = dates // groups
    for k in range(blocks):

        def one_date(d, carry, k=k):
            real, imag = [], []
            for r in range(extent):
                a_re = jnp.broadcast_to(row(0, r, 0, d), (dates, breadth))
                a_im = jnp.broadcast_to(row(0, r, 1, d), (dates, breadth))
                b_re, b_im = row(k, r, 0), row(k, r, 1)
                real.append(a_re * b_re + a_im * b_im)
                imag.append(a_im * b_re - a_re * b_im)
            for part, values in ((0, real), (1, imag)):
                sums = column_sums(window_sums(values, reach, height), band)
                for r in range(height):
                    scale = inverse[0, r, pl.ds(d, 1), :] * inverse[k, r]
                    found[part, k, d, pl.ds(r, dates, stride=height), :] = (
                        sums[r * dates : (r + 1) * dates] * scale
                    )
            return carry

        for g in range(groups):
            lax.fori_loop(g * step, (g + 1) * step, one_date, 0, unroll=min(unroll, step))
            for part in range(2):
                span = pl.ds(g * step, step)
                copy = pltpu.make_async_copy(
                    found.at[part, k, span], out_ref.at[part, k, span], sems.at[k, g, part]
                )
                copy.start()
                copies.append(copy)
    for copy in copies:
        copy.wait()


def coherence_of(axis, outers, rests, even, odd, groups=2, unroll=4):
    blocks = len(outers)
    _, _, dates, breadth = outers[0].shape
    height = rests[0].shape[0] + row_reach

    def body(*refs):
        kernel_body(blocks, axis, groups, unroll, *refs)

    pairs = blocks * dates * dates * height * breadth
    result = (2, blocks, dates, dates * height, breadth)
    return pl.pallas_call(
        body,
        out_shape=jax.ShapeDtypeStruct(result, jnp.float32),
        in_specs=[pl.BlockSpec(memory_space=pltpu.VMEM)] * (2 * blocks + 2),
        out_specs=pl.BlockSpec(memory_space=pl.ANY),
        scratch_shapes=[
            pltpu.VMEM((blocks, height + 2 * row_reach, 2, dates, breadth), jnp.float32),
            pltpu.VMEM((blocks, height, dates, breadth), jnp.float32),
            pltpu.VMEM(result, jnp.float32),
            pltpu.SemaphoreType.DMA((blocks, groups, 2)),
        ],
        compiler_params=pltpu.CompilerParams(vmem_limit_bytes=16 * 1024 * 1024),
        cost_estimate=pl.CostEstimate(
            flops=pairs * 40, bytes_accessed=pairs * 8, transcendentals=0
        ),
    )(*outers, *rests, even, odd)


def passed_along(value, axis, steps):
    count = lax.axis_size(axis)
    pairs = [(source, (source + steps) % count) for source in range(count)]
    return lax.ppermute(value, axis, pairs)


def swapped(value, axis, first):
    count = lax.axis_size(axis)
    pairs = []
    for i in range(first, count - 1, 2):
        pairs += [(i, i + 1), (i + 1, i)]
    if first and count % 2 == 0 and count > 2:
        pairs += [(0, count - 1), (count - 1, 0)]
    return lax.ppermute(value, axis, pairs)


def on_device(acquired):
    height = acquired.shape[2]
    by_row = jnp.transpose(acquired, (2, 0, 1, 3))
    odd_tile = lax.rem(lax.axis_index("tile"), 2) == 1
    head, tail = by_row[:row_reach], by_row[height - row_reach :]
    outer = jnp.where(odd_tile, tail, head)
    rest = jnp.where(odd_tile, by_row[: height - row_reach], by_row[row_reach:])
    outers, rests = [outer], [rest]
    for s in range(1, SHIFTS):
        outers.append(passed_along(outer, "date", -s))
        rests.append(passed_along(rest, "date", -s))
    inner = height - 2 * row_reach
    odd = swapped(jnp.stack(outers), "tile", 1)
    near = [jnp.where(odd_tile, r[:row_reach], r[inner:]) for r in rests]
    even = swapped(jnp.stack(near), "tile", 0)
    found = coherence_of("tile", outers, rests, even, odd)
    parts, shifts, dates = found.shape[:3]
    return found.reshape(parts, shifts, dates, dates, height, found.shape[-1])


def solution(mesh):
    in_specs = (P(None, "date", ("groups", "tile"), None),)
    out_specs = P(None, None, "date", None, ("groups", "tile"), None)
    return jax.shard_map(
        on_device, mesh=mesh, in_specs=in_specs, out_specs=out_specs, check_vma=False
    )
```

```python
import jax
import jax.numpy as jnp
from jax import lax
from jax.experimental import pallas as pl
from jax.experimental.pallas import tpu as pltpu
from jax.sharding import PartitionSpec as P


SHIFTS = 4


row_reach = 5
col_reach = 2


def column_sums(rows, band):
    value = jnp.concatenate(rows, axis=0)
    high = value.astype(jnp.bfloat16)
    low = (value - high.astype(jnp.float32)).astype(jnp.bfloat16)
    return jnp.dot(
        jnp.concatenate([high, low], axis=1), band, preferred_element_type=jnp.float32
    )


def own_windows(rows):
    reach = 2 * row_reach + 1
    total = len(rows)
    last = (total - 1) // reach * reach
    suffix, prefix = {}, {}
    for start in range(0, total, reach):
        stop = min(start + reach, total)
        prefix[start] = rows[start]
        for i in range(start + 1, stop):
            prefix[i] = prefix[i - 1] + rows[i]
        suffix[stop - 1] = rows[stop - 1]
        if stop - start == reach:
            for i in range(stop - 2, start, -1):
                suffix[i] = suffix[i + 1] + rows[i]
    first = [prefix[row_reach + i] for i in range(row_reach)]
    whole = []
    for i in range(total - reach + 1):
        if i % reach == 0:
            whole.append(prefix[i + reach - 1])
        else:
            whole.append(suffix[i] + prefix[i + reach - 1])
    end = []
    for i in range(total - 2 * row_reach, total - row_reach):
        if last - reach < i < last:
            end.append(suffix[i] + prefix[total - 1])
        else:
            tail = rows[i]
            for at in range(i + 1, total):
                tail = tail + rows[at]
            end.append(tail)
    return first, whole, end


def with_halo(first, end, above, below):
    sums = [None] * row_reach
    tail = above[row_reach - 1]
    for i in range(row_reach - 1, -1, -1):
        if i < row_reach - 1:
            tail = tail + above[i]
        sums[i] = first[i] + tail
    lead = below[0]
    for i in range(row_reach):
        if i:
            lead = lead + below[i]
        sums.append(end[i] + lead)
    return sums


def band_of(breadth):
    left = lax.rem(lax.broadcasted_iota(jnp.int32, (2 * breadth, breadth), 0), breadth)
    right = lax.broadcasted_iota(jnp.int32, (2 * breadth, breadth), 1)
    return (jnp.abs(left - right) <= col_reach).astype(jnp.bfloat16)


def products(anchor, partner, date, count):
    shape = partner(0, 0).shape
    real, imag = [], []
    for r in range(count):
        a_re = jnp.broadcast_to(anchor(r, 0, pl.ds(date, 1)), shape)
        a_im = jnp.broadcast_to(anchor(r, 1, pl.ds(date, 1)), shape)
        b_re, b_im = partner(r, 0), partner(r, 1)
        real.append(a_re * b_re + a_im * b_im)
        imag.append(a_im * b_re - a_re * b_im)
    return real, imag


def squares(partner, count):
    found = []
    for r in range(count):
        re, im = partner(r, 0), partner(r, 1)
        found.append(re * re + im * im)
    return found


def reader(ref, *lead):
    def read(r, part, at=slice(None)):
        return ref[(*lead, r, part, at, slice(None))]

    return read


def inner_kernel(axis, together, *refs):
    anchor_outer, anchor_rest, outer, rest = refs[:4]
    whole_ref, partial_ref, power_ref, field, inverse = refs[4:]
    _, _, dates, breadth = outer.shape
    inner = rest.shape[0]
    height = inner + row_reach
    odd_tile = lax.rem(lax.axis_index(axis), 2)
    band = band_of(breadth)
    outer_at = odd_tile * inner
    rest_at = (1 - odd_tile) * row_reach
    for side, (near, far) in enumerate(((anchor_outer, anchor_rest), (outer, rest))):
        field[side, pl.ds(outer_at, row_reach)] = near[...]
        field[side, pl.ds(rest_at, inner)] = far[...]
    anchor, partner = reader(field, 0), reader(field, 1)

    for side in range(2):
        first, whole, end = own_windows(squares(reader(field, side), height))
        power = lax.rsqrt(column_sums(whole, band))
        inverse[side] = power.reshape(len(whole), dates, breadth)
    for i, value in enumerate(first + end):
        power_ref[i] = value

    def some_dates(step, carry):
        wholes = []
        for d in [step * together + i for i in range(together)]:
            for part, values in enumerate(products(anchor, partner, d, height)):
                first, whole, end = own_windows(values)
                wholes += whole
                for i, value in enumerate(first + end):
                    partial_ref[d, part, i] = value
        sums = column_sums(wholes, band)
        count = inverse.shape[1]
        for n, d in enumerate([step * together + i for i in range(together)]):
            for i in range(count):
                scale = inverse[0, i, pl.ds(d, 1), :] * inverse[1, i]
                for part in range(2):
                    at = ((2 * n + part) * count + i) * dates
                    whole_ref[d, part, i] = sums[at : at + dates] * scale
        return carry

    lax.fori_loop(0, dates // together, some_dates, 0, unroll=dates // together)


def inner_part(axis, anchor, partner, together=2):
    _, _, dates, breadth = anchor[0].shape
    height = anchor[1].shape[0] + row_reach
    whole = height - 2 * row_reach
    edge = 2 * row_reach
    outs = ((dates, 2, whole, dates, breadth), (dates, 2, edge, dates, breadth), (edge, dates, breadth))
    work = dates * dates * height * breadth * 24
    on_chip = pl.BlockSpec(memory_space=pltpu.VMEM)
    return pl.pallas_call(
        lambda *refs: inner_kernel(axis, together, *refs),
        out_shape=[jax.ShapeDtypeStruct(shape, jnp.float32) for shape in outs],
        in_specs=[on_chip] * 4,
        out_specs=[on_chip] * 3,
        scratch_shapes=[
            pltpu.VMEM((2, height, 2, dates, breadth), jnp.float32),
            pltpu.VMEM((2, whole, dates, breadth), jnp.float32),
        ],
        compiler_params=pltpu.CompilerParams(vmem_limit_bytes=8 * 1024 * 1024),
        cost_estimate=pl.CostEstimate(flops=work, bytes_accessed=work, transcendentals=0),
    )(*anchor, *partner)


def closing_kernel(blocks, axis, groups, together, *refs):
    whole_refs, partial_refs = refs[:blocks], refs[blocks : 2 * blocks]
    power_refs = refs[2 * blocks : 3 * blocks]
    even_ref, odd_ref, out_ref, halo, inverse, found, sems = refs[3 * blocks :]
    dates, _, whole, _, breadth = whole_refs[0].shape
    height = whole + 2 * row_reach
    edge = 2 * row_reach
    pitch = found.shape[3] // dates
    here = lax.axis_index(axis)
    count = lax.axis_size(axis)
    odd_tile = lax.rem(here, 2)
    band = band_of(breadth)

    even_live = jnp.where(here == count - 1, odd_tile, 1) == 1
    odd_live = jnp.where(odd_tile == 0, here > 0, here < count - 1)
    even_at = (1 - odd_tile) * row_reach
    odd_at = odd_tile * row_reach

    def finished(partial, values):
        first = [partial[i] for i in range(row_reach)]
        end = [partial[i] for i in range(row_reach, edge)]
        return with_halo(first, end, values[:row_reach], values[row_reach:])

    rows = [*range(row_reach), *range(height - row_reach, height)]
    copies = []
    by_date = found.reshape(2, blocks, dates, dates, pitch, breadth)
    step = dates // groups
    for k in range(blocks):
        even, odd = even_ref[k], odd_ref[k]
        halo[k, pl.ds(even_at, row_reach)] = jnp.where(even_live, even, jnp.zeros_like(even))
        halo[k, pl.ds(odd_at, row_reach)] = jnp.where(odd_live, odd, jnp.zeros_like(odd))
        sums = finished(power_refs[k], squares(reader(halo, k), edge))
        inverse[k] = lax.rsqrt(column_sums(sums, band)).reshape(edge, dates, breadth)

        def some_dates(at, carry, k=k):
            several = [at * together + i for i in range(together)]
            sums = []
            for d in several:
                pair = products(reader(halo, 0), reader(halo, k), d, edge)
                for part, values in enumerate(pair):
                    sums += finished(partial_refs[k].at[d, part], values)
                    for i in range(whole):
                        to = pl.ds(row_reach + i, dates, stride=pitch)
                        found[part, k, d, to, :] = whole_refs[k][d, part, i]
            sums = column_sums(sums, band)
            for n, d in enumerate(several):
                for i, r in enumerate(rows):
                    scale = inverse[0, i, pl.ds(d, 1), :] * inverse[k, i]
                    for part in range(2):
                        start = ((2 * n + part) * edge + i) * dates
                        found[part, k, d, pl.ds(r, dates, stride=pitch), :] = (
                            sums[start : start + dates] * scale
                        )
            return carry

        turns = step // together
        for g in range(groups):
            lax.fori_loop(g * turns, (g + 1) * turns, some_dates, 0, unroll=turns)
            for part in range(2):
                span = pl.ds(g * step, step)
                copy = pltpu.make_async_copy(
                    by_date.at[part, k, span, :, pl.ds(0, height)],
                    out_ref.at[part, k, span],
                    sems.at[k, g, part],
                )
                copy.start()
                copies.append(copy)
    for copy in copies:
        copy.wait()


def closing_part(axis, wholes, partials, powers, even, odd, groups=2, together=2):
    blocks = len(wholes)
    dates, _, whole, _, breadth = wholes[0].shape
    height = whole + 2 * row_reach
    edge = 2 * row_reach
    result = (2, blocks, dates, dates, height, breadth)
    pitch = height + 8
    work = blocks * dates * dates * height * breadth * 12
    return pl.pallas_call(
        lambda *refs: closing_kernel(blocks, axis, groups, together, *refs),
        out_shape=jax.ShapeDtypeStruct(result, jnp.float32),
        in_specs=[pl.BlockSpec(memory_space=pltpu.VMEM)] * (3 * blocks + 2),
        out_specs=pl.BlockSpec(memory_space=pl.ANY),
        scratch_shapes=[
            pltpu.VMEM((blocks, edge, 2, dates, breadth), jnp.float32),
            pltpu.VMEM((blocks, edge, dates, breadth), jnp.float32),
            pltpu.VMEM((2, blocks, dates, dates * pitch, breadth), jnp.float32),
            pltpu.SemaphoreType.DMA((blocks, groups, 2)),
        ],
        compiler_params=pltpu.CompilerParams(vmem_limit_bytes=16 * 1024 * 1024),
        cost_estimate=pl.CostEstimate(flops=work, bytes_accessed=work, transcendentals=0),
    )(*wholes, *partials, *powers, even, odd)


def passed_along(value, axis, steps):
    count = lax.axis_size(axis)
    pairs = [(source, (source + steps) % count) for source in range(count)]
    return lax.ppermute(value, axis, pairs)


def swapped(value, axis, first):
    count = lax.axis_size(axis)
    pairs = []
    for i in range(first, count - 1, 2):
        pairs += [(i, i + 1), (i + 1, i)]
    if first and count % 2 == 0 and count > 2:
        pairs += [(0, 0), (count - 1, count - 1)]
    return lax.ppermute(value, axis, pairs)


def on_device(acquired):
    height = acquired.shape[2]
    by_row = jnp.transpose(acquired, (2, 0, 1, 3))
    odd_tile = lax.rem(lax.axis_index("tile"), 2) == 1
    head, tail = by_row[:row_reach], by_row[height - row_reach :]
    outer = jnp.where(odd_tile, tail, head)
    rest = jnp.where(odd_tile, by_row[: height - row_reach], by_row[row_reach:])
    outers, rests = [outer], [rest]
    for s in range(1, SHIFTS):
        outers.append(passed_along(outer, "date", -s))
        rests.append(passed_along(rest, "date", -s))
    inner = height - 2 * row_reach
    odd = swapped(jnp.stack(outers), "tile", 1)
    near = [jnp.where(odd_tile, r[:row_reach], r[inner:]) for r in rests]
    even = swapped(jnp.stack(near), "tile", 0)
    parts = []
    for s in range(SHIFTS):
        parts.append(inner_part("tile", (outer, rest), (outers[s], rests[s])))
    return closing_part("tile", *zip(*parts), even, odd)


def solution(mesh):
    in_specs = (P(None, "date", ("groups", "tile"), None),)
    out_specs = P(None, None, "date", None, ("groups", "tile"), None)
    return jax.shard_map(
        on_device, mesh=mesh, in_specs=in_specs, out_specs=out_specs, check_vma=False
    )
```
